512 devices in a mesh: dp: 32 (over z_lo, x), mp: 16 (over y, z_hi, core).
Axes of the slice: x: 4, y: 4, z: 16 (z_hi: 2, z_lo: 8; z = z_hi * 8 + z_lo), core: 2. Of those that a mesh axis runs over, the one named last changes fastest.
Arguments:
- hidden: bfloat16 [512, 4096], P('dp'), may hold values from -6 to 6
- wq_direct: bfloat16 [4096, 2048], P(None, 'mp'), may hold values from -0.09375 to 0.09375
- wkv_direct: bfloat16 [2, 4096, 2048], P(None, None, 'mp'), may hold values from -0.09375 to 0.09375
- wo_direct: bfloat16 [2048, 4096], P(None, 'mp'), may hold values from -0.125 to 0.125
- kv_cache: bfloat16 [2, 512, 32, 2048], P(None, 'dp', None, 'mp'), may hold values from -6 to 6
- parent: int32 [512], P('dp'), may hold values from 0 to 15
- lengths: int32 [512], P('dp'), may hold values from 1 to 32
- cand_embed: bfloat16 [512, 32, 4096], P('dp', None, 'mp'), may hold values from -6 to 6
- source: bfloat16 [32, 8, 4096], P('dp', None, 'mp'), may hold values from -6 to 6
- enc_qkv: bfloat16 [3, 4096, 2048], P(None, 'dp', 'mp'), may hold values from -0.09375 to 0.09375
- enc_out: bfloat16 [2048, 4096], P('dp', 'mp'), may hold values from -0.125 to 0.125
- cross_q: bfloat16 [4096, 2048], P('dp', 'mp'), may hold values from -0.09375 to 0.09375
- cross_kv: bfloat16 [2, 4096, 2048], P(None, 'dp', 'mp'), may hold values from -0.09375 to 0.09375
- cross_out: bfloat16 [2048, 4096], P('dp', 'mp'), may hold values from -0.125 to 0.125
- w_direct: bfloat16 [4096], P('mp'), may hold values from -0.09375 to 0.09375
- w_channel: bfloat16 [4096], P('mp'), may hold values from -0.09375 to 0.09375
- target_shard: int32 [512], P('dp'), may hold values from 0 to 31, as said below
Outputs:
- direct_state: bfloat16 [512, 4096], P('dp', 'mp')
- rerank_score: float32 [512], P('dp')
- channel_score: float32 [512], P('dp')
The draws below stay inside these ranges and needn't reach their ends.
Inputs may be any that keep to these rules, and one draw needn't show every extreme that they name: `target_shard`: every shard receives exactly one candidate of each beam index; a device sends exactly 1 of its candidates to each shard that it sends to.
All inputs are finite; a program needn't handle non-finite values.
Results may differ from the reference program's by a relative error of at most 0.0075.
Values may be sent and summed in bfloat16 or wider, within the bound.
A program may use at most 128 MiB of HBM per device.

```python
import math
import jax
import jax.numpy as jnp
from jax import lax

D = 4096
HD = 64
BEAMS = 16
LEN = 32
SRC_LEN = 8
HW = 2048
SOURCES = 32
CANDS = 512
N_DP = 32


def draw_target_shard(key, part):
    spread = min(BEAMS, N_DP)
    order = jax.random.permutation(jax.random.fold_in(key, 11), N_DP).astype(jnp.int32)
    values = jnp.arange(N_DP, dtype=jnp.int32)
    rank_of = jnp.zeros((N_DP,), jnp.int32).at[order].set(values)
    special = (values == N_DP - 1) | (values == 1) | (values == N_DP // 2)
    priority = rank_of + N_DP * (1 - special.astype(jnp.int32))
    chosen = jnp.argsort(priority, stable=True)[:spread].astype(jnp.int32)
    shuffle = jax.random.permutation(jax.random.fold_in(key, 13), spread).astype(jnp.int32)
    offsets = chosen[shuffle]
    cand_index = jnp.arange(BEAMS * N_DP, dtype=jnp.int32)
    return ((cand_index // BEAMS + offsets[cand_index % BEAMS % spread]) % N_DP).astype(jnp.int32)


def place_ends(result, stream_key, low, largest):
    index_at = [jax.random.randint(jax.random.fold_in(stream_key, axis), (), 0, length) for axis, length in enumerate(result.shape)]
    longest = result.shape.index(max(result.shape))
    next_to = index_at[:longest] + [(index_at[longest] + 1) % result.shape[longest]] + index_at[longest + 1:]
    return result.at[tuple(index_at)].set(low).at[tuple(next_to)].set(largest)


def block_scale(stream_key, dims, split, low, top_value):
    def one(axis_at, parts):
        steps = jax.random.uniform(jax.random.fold_in(jax.random.fold_in(stream_key, 6), axis_at), (parts,), jnp.float32, low / len(split), top_value / len(split))
        return jnp.repeat(jnp.exp(steps), dims[axis_at] // parts).reshape((-1,) + (1,) * (len(dims) - axis_at - 1))

    loudness = one(*split[0])
    for cut in split[1:]:
        loudness = loudness * one(*cut)
    return loudness


def bell_draw(stream_key, shape, width, bound, split=(), held_as=jnp.bfloat16):
    loudness = block_scale(stream_key, shape, split, -0.22, 0.18) if split else 1.0
    drawn = jax.random.normal(stream_key, shape, jnp.float32) * width * loudness
    return jnp.minimum(jnp.maximum(drawn, -bound), bound).astype(held_as)


def setup_inputs(seed: int = 0) -> dict:
    splits = jax.random.split(jax.random.key(seed), 18)
    hidden = bell_draw(splits[0], (CANDS, D), 1.0, 6.0, ((0, 32),))
    wq_direct = bell_draw(splits[1], (D, HW), D ** -0.5, 0.09375, ((1, 16),))
    wkv_direct = bell_draw(splits[2], (2, D, HW), D ** -0.5, 0.09375, ((2, 16),))
    wo_direct = bell_draw(splits[3], (HW, D), HW ** -0.5, 0.125, ((1, 16),))
    kv_cache = bell_draw(splits[4], (2, CANDS, LEN, HW), 1.0, 6.0, ((1, 32), (3, 16)))
    parent = place_ends(jax.random.randint(splits[5], (CANDS,), 0, BEAMS), jax.random.fold_in(splits[5], 1), 0, BEAMS - 1).astype(jnp.int32)
    lengths = place_ends(jax.random.randint(splits[6], (CANDS,), 1, LEN + 1), jax.random.fold_in(splits[6], 1), 1, LEN).astype(jnp.int32)
    cand_embed = bell_draw(splits[7], (CANDS, LEN, D), 1.0, 6.0, ((0, 32), (2, 16)))
    source = bell_draw(splits[8], (SOURCES, SRC_LEN, D), 1.0, 6.0, ((0, 32), (2, 16)))
    enc_qkv = bell_draw(splits[9], (3, D, HW), D ** -0.5, 0.09375, ((1, 32), (2, 16)))
    enc_out = bell_draw(splits[10], (HW, D), HW ** -0.5, 0.125, ((0, 32), (1, 16)))
    cross_q = bell_draw(splits[11], (D, HW), D ** -0.5, 0.09375, ((0, 32), (1, 16)))
    cross_kv = bell_draw(splits[12], (2, D, HW), D ** -0.5, 0.09375, ((1, 32), (2, 16)))
    cross_out = bell_draw(splits[13], (HW, D), HW ** -0.5, 0.125, ((0, 32), (1, 16)))
    w_direct = bell_draw(splits[14], (D,), D ** -0.5, 0.09375, ((0, 16),))
    w_channel = bell_draw(splits[15], (D,), D ** -0.5, 0.09375, ((0, 16),))
    target_shard = draw_target_shard(jax.random.fold_in(splits[17], 71), 0)
    return {"hidden": hidden, "wq_direct": wq_direct, "wkv_direct": wkv_direct, "wo_direct": wo_direct, "kv_cache": kv_cache, "parent": parent, "lengths": lengths, "cand_embed": cand_embed, "source": source, "enc_qkv": enc_qkv, "enc_out": enc_out, "cross_q": cross_q, "cross_kv": cross_kv, "cross_out": cross_out, "w_direct": w_direct, "w_channel": w_channel, "target_shard": target_shard}


EPSILON = 1e-06

def attend(queries, keys, values, valid):
    group_n, query_n, columns = queries.shape
    key_n = keys.shape[1]
    head_n = columns // HD
    query_heads = queries.reshape(group_n, query_n, head_n, HD).astype(jnp.float32)
    key_heads = keys.reshape(group_n, key_n, head_n, HD).astype(jnp.float32)
    value_heads = values.reshape(group_n, key_n, head_n, HD).astype(jnp.float32)
    scores = jnp.einsum('bqhd,bkhd->bhqk', query_heads, key_heads) / math.sqrt(HD)
    scores = jnp.where(valid[:, None, None, :], scores, -1e+30)
    weights = jax.nn.softmax(scores, axis=-1).astype(jnp.bfloat16)
    context = jnp.einsum('bhqk,bkhd->bqhd', weights.astype(jnp.float32), value_heads)
    return context.astype(jnp.bfloat16).reshape(group_n, query_n, columns)

def project(rows, matrix):
    return jnp.dot(rows, matrix, preferred_element_type=jnp.float32)

def normalized(values):
    return jnp.sqrt(lax.optimization_barrier(jnp.mean(values * values, axis=-1)) + EPSILON)

def reference(hidden, wq_direct, wkv_direct, wo_direct, kv_cache, parent, lengths, cand_embed, source, enc_qkv, enc_out, cross_q, cross_kv, cross_out, w_direct, w_channel, target_shard):
    cand_index = jnp.arange(CANDS, dtype=jnp.int32)
    parent_row = cand_index // BEAMS * BEAMS + parent
    query_new = project(hidden, wq_direct).astype(jnp.bfloat16)
    key_new = project(hidden, wkv_direct[0]).astype(jnp.bfloat16)
    value_new = project(hidden, wkv_direct[1]).astype(jnp.bfloat16)
    all_keys = jnp.concatenate([kv_cache[0][parent_row], key_new[:, None]], axis=1)
    all_values = jnp.concatenate([kv_cache[1][parent_row], value_new[:, None]], axis=1)
    positions = jnp.arange(LEN, dtype=jnp.int32)
    cache_valid = jnp.concatenate([positions[None, :] < lengths[:, None], jnp.ones((CANDS, 1), dtype=bool)], axis=1)
    context = attend(query_new[:, None], all_keys, all_values, cache_valid)[:, 0]
    new_state = hidden.astype(jnp.float32) + project(context, wo_direct)
    direct_score = lax.optimization_barrier(jnp.sum(new_state * w_direct.astype(jnp.float32), axis=1)) / normalized(new_state)

    def score_source(source_id):
        rows_here = lax.dynamic_slice_in_dim(parent_row, source_id * BEAMS, BEAMS)
        lens_here = lax.dynamic_slice_in_dim(lengths, source_id * BEAMS, BEAMS)
        token_rows = cand_embed[rows_here].reshape(BEAMS * LEN, D)
        enc_queries = project(token_rows, enc_qkv[0]).astype(jnp.bfloat16).reshape(BEAMS, LEN, HW)
        enc_keys = project(token_rows, enc_qkv[1]).astype(jnp.bfloat16).reshape(BEAMS, LEN, HW)
        enc_values = project(token_rows, enc_qkv[2]).astype(jnp.bfloat16).reshape(BEAMS, LEN, HW)
        key_valid = positions[None, :] < lens_here[:, None]
        enc_context = attend(enc_queries, enc_keys, enc_values, key_valid).reshape(BEAMS * LEN, HW)
        summed = token_rows.astype(jnp.float32) + project(enc_context, enc_out)
        memory = (summed / normalized(summed)[:, None]).astype(jnp.bfloat16)
        cross_keys = project(memory, cross_kv[0]).astype(jnp.bfloat16).reshape(BEAMS, LEN, HW)
        cross_values = project(memory, cross_kv[1]).astype(jnp.bfloat16).reshape(BEAMS, LEN, HW)
        own_source = lax.dynamic_index_in_dim(source, source_id, 0, keepdims=False)
        queries_once = project(own_source, cross_q).astype(jnp.bfloat16)
        cross_queries = jnp.broadcast_to(queries_once[None], (BEAMS, SRC_LEN, HW))
        cross_context = attend(cross_queries, cross_keys, cross_values, key_valid).reshape(BEAMS * SRC_LEN, HW)
        source_rows = jnp.broadcast_to(own_source[None].astype(jnp.float32), (BEAMS, SRC_LEN, D)).reshape(BEAMS * SRC_LEN, D)
        decoded = source_rows + project(cross_context, cross_out)
        position_score = lax.optimization_barrier(jnp.sum(decoded * w_channel.astype(jnp.float32), axis=1)) / normalized(decoded)
        return lax.optimization_barrier(jnp.mean(position_score.reshape(BEAMS, SRC_LEN), axis=1))
    cand_channel = lax.map(score_source, jnp.arange(N_DP, dtype=jnp.int32)).reshape(CANDS)
    slot_index = target_shard * BEAMS + cand_index % BEAMS
    channel_score = jnp.zeros((CANDS,), jnp.float32).at[slot_index].set(cand_channel)
    rerank_score = direct_score + cand_channel
    return (new_state.astype(jnp.bfloat16), rerank_score, channel_score)
```

```python
import functools
import math

import jax
import jax.numpy as jnp
from jax import lax
from jax.experimental import pallas as pl
from jax.experimental.pallas import tpu as pltpu
from jax.sharding import Mesh
from jax.sharding import PartitionSpec as P

D = 4096
HD = 64
EPSILON = 1e-06
AX = ("zl", "x", "y", "zh", "c")
ZL, X, Y, ZH, C = 8, 4, 4, 2, 2
MP = ("y", "zh", "c")
DP = ("zl", "x")
VMEM = pltpu.VMEM
MESH = pl.DeviceIdType.MESH
FLOWS_MP = 22
FLOWS_DP = 74


def hint(value, step):
    return pl.multiple_of(value, step)


class Links:
    def __init__(self, send, recv):
        self.send, self.recv, self.count, self.open = send, recv, 0, []

    def slot(self):
        self.count += 1
        return self.count - 1

    def copy(self, slot, src, dst, to):
        return pltpu.make_async_remote_copy(
            src_ref=src,
            dst_ref=dst,
            send_sem=self.send.at[slot],
            recv_sem=self.recv.at[slot],
            device_id=to,
            device_id_type=MESH,
        )

    def go(self, src, dst, to):
        flow = self.copy(self.slot(), src, dst, to)
        flow.start()
        self.open.append(flow)
        return flow


def gather_kernel(mp, dp, *refs):
    n_mp, n_dp = len(mp), len(dp)
    mp_in, dp_in = refs[:n_mp], refs[n_mp : n_mp + n_dp]
    mp_out = refs[n_mp + n_dp : 2 * n_mp + n_dp]
    dp_out = refs[2 * n_mp + n_dp : 2 * n_mp + 2 * n_dp]
    send, recv, local = refs[2 * (n_mp + n_dp) :]
    zl, x, y, zh, c = (lax.axis_index(a) for a in AX)
    links = Links(send, recv)
    yr, yl, y2 = lax.rem(y + 1, Y), lax.rem(y + Y - 1, Y), lax.rem(y + 2, Y)
    xr, xl = lax.rem(x + 1, X), lax.rem(x + X - 1, X)
    other = 1 - zh
    partner = 1 - c

    barrier = pltpu.get_barrier_semaphore()

    def greet(to):
        pl.semaphore_signal(barrier, inc=1, device_id=to, device_id_type=MESH)

    if n_mp:
        for to in ({"zh": other}, {"y": yr}, {"y": yl}, {"c": partner}):
            greet(to)
    if n_dp:
        greet({"x": xr})
        greet({"x": xl})

        place = zh * ZL + zl
        for step in (1, ZL * ZH - 1):
            near = lax.rem(place + step, ZL * ZH)
            greet({"zh": near // ZL, "zl": lax.rem(near, ZL)})

    homes = []
    for k in range(n_mp):
        width = mp_in[k].shape[1]
        at = hint(((y * ZH + zh) * C + c) * width, 128)
        homes.append(
            pltpu.make_async_copy(mp_in[k], mp_out[k].at[:, pl.ds(at, width)], local.at[k])
        )
    for k in range(n_dp):
        rows = dp_in[k].shape[1]
        at = hint((zl * X + x) * rows, 16)
        homes.append(
            pltpu.make_async_copy(
                dp_in[k], dp_out[k].at[:, pl.ds(at, rows)], local.at[n_mp + k]
            )
        )
    for home in homes:
        home.start()
    pl.semaphore_wait(barrier, 4 * (n_mp > 0) + 4 * (n_dp > 0))

    tasks = []
    arrivals = []
    guarded = []

    def at_time(when, task):
        tasks.append((when, len(tasks), task))

    def mp_chunk(k, r0, n, scale, z_time):
        width = mp_in[k].shape[1]
        half = n // 2

        def full(start, size, yy, hh):
            at = hint(((yy * ZH + hh) * C + c) * width, 128)
            return mp_out[k].at[pl.ds(start, size), pl.ds(at, width)]

        kept = {}

        def to_core(start, size, yy, hh):
            block = full(start, size, yy, hh)
            arrivals.append(links.go(block, block, {"c": partner}))

        def first():
            src = mp_in[k].at[pl.ds(r0, n)]
            dst = full(r0, n, y, zh)
            kept["z"] = links.go(src, dst, {"zh": other})
            kept["r", 0] = links.go(src, dst, {"y": yr})
            kept["l", 0] = links.go(src, dst, {"y": yl})
            arrivals.append(links.go(src, dst, {"c": partner}))

        def second(phase):
            hh = (zh, other)[phase]
            kept["r", phase].wait_recv()
            block = full(r0, half, yl, hh)
            kept["or", phase] = links.go(block, block, {"y": yr})
            to_core(r0, n, yl, hh)
            kept["l", phase].wait_recv()
            block = full(r0 + half, half, yr, hh)
            kept["ol", phase] = links.go(block, block, {"y": yl})
            to_core(r0, n, yr, hh)

        def third(phase):
            hh = (zh, other)[phase]
            kept["or", phase].wait_recv()
            to_core(r0, half, y2, hh)
            kept["ol", phase].wait_recv()
            to_core(r0 + half, half, y2, hh)

        def crossed():
            kept["z"].wait_recv()
            block = full(r0, n, y, other)
            kept["r", 1] = links.go(block, block, {"y": yr})
            kept["l", 1] = links.go(block, block, {"y": yl})
            to_core(r0, n, y, other)

        at_time(-1.0 + r0 * 1e-4, first)
        at_time(scale * (r0 / n + 1), lambda: second(0))
        at_time(scale * (r0 / n + 2), lambda: third(0))
        at_time(z_time, crossed)
        at_time(z_time + scale + 1, lambda: second(1))
        at_time(z_time + 2 * scale + 2, lambda: third(1))

    def dp_array(k, z_step, x_step):
        rows = dp_in[k].shape[1]
        half = rows // 2

        def full(b, xx, start, size):
            at = hint((b * X + xx) * rows + start, 16)
            return dp_out[k].at[:, pl.ds(at, size)]

        z_slots = {(way, s): links.slot() for way in (1, -1) for s in range(ZL - 1)}

        def held(way, s):
            return zl - way * s

        def has(way, s):
            return zl - s >= 0 if way > 0 else zl + s <= ZL - 1

        def room(way):
            return zl < ZL - 1 if way > 0 else zl > 0

        def z_flow(way, s):
            b = held(way, s)
            block = full(b, x, 0, rows)
            src = dp_in[k] if s == 0 else block
            return links.copy(z_slots[way, s], src, block, {"zl": zl + way})

        def z_send(way, s):
            cond = jnp.logical_and(has(way, s), room(way))
            pl.when(cond)(lambda: z_flow(way, s).start())
            guarded.append((cond, lambda: z_flow(way, s).wait_send()))

        def x_block(cond, b, src, when):
            slots = [links.slot() for _ in range(4)]

            def near(way):
                block = full(b, x, 0, rows)
                return links.copy(
                    slots[0 if way > 0 else 1],
                    block if src is None else src,
                    block,
                    {"x": xr if way > 0 else xl},
                )

            def far(way):
                block = full(b, xl if way > 0 else xr, 0 if way > 0 else half, half)
                return links.copy(
                    slots[2 if way > 0 else 3], block, block, {"x": xr if way > 0 else xl}
                )

            def start():
                near(1).start()
                near(-1).start()

            def forward():
                near(1).wait_recv()
                far(1).start()
                near(-1).wait_recv()
                far(-1).start()

            def finish():
                for way in (1, -1):
                    far(way).wait_recv()
                    near(way).wait_send()
                    far(way).wait_send()

            run = (lambda f: f()) if cond is None else (lambda f: pl.when(cond)(f))
            at_time(when + x_step, lambda: run(forward))
            at_time(1e6, lambda: run(finish))
            return start

        def begin():
            for way in (1, -1):
                z_send(way, 0)

        own_start = x_block(None, zl, dp_in[k], 0.0)
        at_time(-2.0 + 0.01 * k, lambda: (begin(), own_start()))

        def z_step_task(way, s):
            cond = has(way, s)
            when = z_step * s
            start = x_block(cond, held(way, s), None, when)

            def task():
                @pl.when(cond)
                def _():
                    block = full(held(way, s), x, 0, rows)
                    links.copy(
                        z_slots[way, s - 1], block, block, {"zl": zl - way}
                    ).wait_recv()

                if s < ZL - 1:
                    z_send(way, s)
                pl.when(cond)(start)

            at_time(when, task)

        for s in range(1, ZL):
            for way in (1, -1):
                z_step_task(way, s)

    for k, spec in enumerate(mp):
        r0 = 0
        for number, n in enumerate(spec["chunks"]):
            mp_chunk(k, r0, n, spec["y_time"], spec["z_time"] * (number + 1))
            r0 += n
    for k, spec in enumerate(dp):
        dp_array(k, spec["z_time"], spec["x_time"])
    for _, _, task in sorted(tasks, key=lambda t: t[:2]):
        task()
    for flow in arrivals:
        flow.wait_recv()
    for flow in links.open:
        flow.wait_send()
    for cond, finish in guarded:
        pl.when(cond)(finish)
    for home in homes:
        home.wait()


def gather(mp_arrays, mp_specs, dp_arrays, dp_specs, collective_id):
    outs = [jax.ShapeDtypeStruct((a.shape[0], a.shape[1] * 16), a.dtype) for a in mp_arrays]
    outs += [
        jax.ShapeDtypeStruct((a.shape[0], a.shape[1] * 32, a.shape[2]), a.dtype)
        for a in dp_arrays
    ]
    slots = FLOWS_MP * sum(len(s["chunks"]) for s in mp_specs) + FLOWS_DP * len(dp_specs)
    count = len(mp_arrays) + len(dp_arrays)
    return pl.pallas_call(
        functools.partial(gather_kernel, mp_specs, dp_specs),
        out_shape=outs,
        in_specs=[pl.BlockSpec(memory_space=VMEM)] * count,
        out_specs=[pl.BlockSpec(memory_space=VMEM)] * count,
        scratch_shapes=[
            pltpu.SemaphoreType.DMA((slots,)),
            pltpu.SemaphoreType.DMA((slots,)),
            pltpu.SemaphoreType.DMA((count,)),
        ],
        compiler_params=pltpu.CompilerParams(
            collective_id=collective_id, has_side_effects=True, vmem_limit_bytes=48 << 20
        ),
        name=f"gather_{collective_id}",
    )(*mp_arrays, *dp_arrays)


def dot(a, b):
    return jnp.dot(a, b, preferred_element_type=jnp.float32)


def dot_t(a, b):
    return lax.dot_general(a, b, (((1,), (1,)), ((), ())), preferred_element_type=jnp.float32)


def of_head(array, head):
    lane = lax.broadcasted_iota(jnp.int32, array.shape, 1)
    return jnp.where((lane >= HD) == (head == 1), array, jnp.zeros_like(array))


def join_heads(first, second):
    lane = lax.broadcasted_iota(jnp.int32, first.shape, 1)
    return jnp.where(lane >= HD, second, first)


def softmax(scores):
    top = jnp.max(scores, axis=1, keepdims=True)
    raised = jnp.exp(scores - top)
    return raised / jnp.sum(raised, axis=1, keepdims=True)


def length_row(lengths, first, count, width):
    col = lax.broadcasted_iota(jnp.int32, (1, width), 1)
    row = jnp.zeros((1, width), jnp.int32)
    for u in range(count):
        row = jnp.where(col // 32 == u, lengths[first + u], row)
    return row


def encoder_kernel(parent, lengths, q, k, v, out):
    group = 4
    for first in range(0, 16, group):
        starts = [hint(parent[first + u] * 32, 32) for u in range(group)]
        queries, keys, values = (
            jnp.concatenate([a[pl.ds(s, 32), :] for s in starts], axis=0) for a in (q, k, v)
        )
        shape = (32 * group, 32 * group)
        row = lax.broadcasted_iota(jnp.int32, shape, 0)
        col = lax.broadcasted_iota(jnp.int32, shape, 1)
        live = (row // 32 == col // 32) & (
            col % 32 < length_row(lengths, first, group, 32 * group)
        )
        heads = []
        for head in range(2):
            scores = dot_t(of_head(queries, head), keys) * (1.0 / math.sqrt(HD))
            weights = softmax(jnp.where(live, scores, -1e30)).astype(jnp.bfloat16)
            heads.append(dot(weights, values))
        out[pl.ds(32 * first, 32 * group), :] = join_heads(*heads).astype(jnp.bfloat16)


def direct_kernel(parent, lengths, q, k, v, cache, out, keys, values):
    for i in range(16):
        keys[pl.ds(32 * i, 32), :] = cache[0, parent[i]]
        values[pl.ds(32 * i, 32), :] = cache[1, parent[i]]
    queries, key_new, value_new = q[...], k[...], v[...].astype(jnp.float32)
    row = lax.broadcasted_iota(jnp.int32, (16, 512), 0)
    col = lax.broadcasted_iota(jnp.int32, (16, 512), 1)
    live = (row == col // 32) & (col % 32 < length_row(lengths, 0, 16, 512))
    heads = []
    for head in range(2):
        mine = of_head(queries, head)
        scores = dot_t(mine, keys[...]) * (1.0 / math.sqrt(HD))
        scores = jnp.where(live, scores, -1e30)
        last = jnp.sum(
            mine.astype(jnp.float32) * key_new.astype(jnp.float32), axis=1, keepdims=True
        ) * (1.0 / math.sqrt(HD))
        top = jnp.maximum(jnp.max(scores, axis=1, keepdims=True), last)
        raised, raised_last = jnp.exp(scores - top), jnp.exp(last - top)
        total = jnp.sum(raised, axis=1, keepdims=True) + raised_last
        weights = (raised / total).astype(jnp.bfloat16)
        weight_last = (raised_last / total).astype(jnp.bfloat16).astype(jnp.float32)
        heads.append(dot(weights, values[...]) + weight_last * value_new)
    out[...] = join_heads(*heads).astype(jnp.bfloat16)


def cross_kernel(lengths, q, k, v, out):
    row = lax.broadcasted_iota(jnp.int32, (128, 512), 0)
    col = lax.broadcasted_iota(jnp.int32, (128, 512), 1)
    live = (row % 16 == col // 32) & (col % 32 < length_row(lengths, 0, 16, 512))
    heads = []
    for head in range(2):
        scores = dot_t(of_head(q[...], head), k[...]) * (1.0 / math.sqrt(HD))
        weights = softmax(jnp.where(live, scores, -1e30)).astype(jnp.bfloat16)
        heads.append(dot(weights, v[...]))
    out[...] = join_heads(*heads).astype(jnp.bfloat16)


def local_call(kernel, out_shape, scalars, arrays, scratch=()):
    return pl.pallas_call(
        kernel,
        out_shape=jax.ShapeDtypeStruct(out_shape, jnp.bfloat16),
        in_specs=[pl.BlockSpec(memory_space=pltpu.SMEM)] * len(scalars)
        + [pl.BlockSpec(memory_space=VMEM)] * len(arrays),
        out_specs=pl.BlockSpec(memory_space=VMEM),
        scratch_shapes=list(scratch),
    )(*scalars, *arrays)


def score_kernel(parts, target, rerank, channel, got, rows, inbox, sends, recvs):
    zl, x, y, zh, c = (lax.axis_index(a) for a in AX)
    me_m = (y * ZH + zh) * C + c
    me_d = zl * X + x
    n_m, n_d = Y * ZH * C, ZL * X

    def to_m(k):
        m = lax.rem(me_m + k, n_m)
        return {"y": m // (ZH * C), "zh": lax.rem(m // C, ZH), "c": lax.rem(m, C)}

    def to_d(k):
        d = lax.rem(me_d + k, n_d)
        return {"zl": d // X, "x": lax.rem(d, X)}

    barrier = pltpu.get_barrier_semaphore()
    for k in range(1, n_m):
        pl.semaphore_signal(barrier, inc=1, device_id=to_m(k), device_id_type=MESH)
    for k in range(1, n_d):
        pl.semaphore_signal(barrier, inc=1, device_id=to_d(k), device_id_type=MESH)
    pl.semaphore_wait(barrier, n_m + n_d - 2)
    flows = []
    for k in range(1, n_m):
        flow = pltpu.make_async_remote_copy(
            src_ref=parts,
            dst_ref=got.at[me_m],
            send_sem=sends.at[k],
            recv_sem=recvs.at[k],
            device_id=to_m(k),
            device_id_type=MESH,
        )
        flow.start()
        flows.append(flow)
    for flow in flows:
        flow.wait_recv()
    total = parts[...]
    for m in range(n_m):
        total = total + jnp.where(me_m == m, 0.0, got[m])
    dots, squares = total[0:8], total[8:16]
    score = jnp.sum(dots / jnp.sqrt(squares / D + EPSILON), axis=0, keepdims=True) / 8
    tail = total[16:24]
    direct = tail[0:1] / jnp.sqrt(tail[1:2] / D + EPSILON)
    rerank[...] = direct + score
    shard = lax.broadcasted_iota(jnp.int32, (n_d, 128), 0)
    slots = jnp.where(shard == target[...], score, 0.0)
    rows[...] = slots
    for k in range(1, n_d):
        d = lax.rem(me_d + k, n_d)
        flow = pltpu.make_async_remote_copy(
            src_ref=rows.at[pl.ds(d, 1)],
            dst_ref=inbox.at[pl.ds(me_d, 1)],
            send_sem=sends.at[n_m + k],
            recv_sem=recvs.at[n_m + k],
            device_id=to_d(k),
            device_id_type=MESH,
        )
        flow.start()
        flows.append(flow)
    for flow in flows[n_m - 1 :]:
        flow.wait_recv()
    mine = shard == me_d
    channel[...] = jnp.sum(jnp.where(mine, slots, inbox[...]), axis=0, keepdims=True)
    for flow in flows:
        flow.wait_send()


def scores(parts, target):
    return pl.pallas_call(
        score_kernel,
        out_shape=[jax.ShapeDtypeStruct((1, 128), jnp.float32)] * 2,
        in_specs=[pl.BlockSpec(memory_space=VMEM)] * 2,
        out_specs=[pl.BlockSpec(memory_space=VMEM)] * 2,
        scratch_shapes=[
            pltpu.VMEM((16, 24, 128), jnp.float32),
            pltpu.VMEM((32, 128), jnp.float32),
            pltpu.VMEM((32, 128), jnp.float32),
            pltpu.SemaphoreType.DMA((48,)),
            pltpu.SemaphoreType.DMA((48,)),
        ],
        compiler_params=pltpu.CompilerParams(collective_id=9, has_side_effects=True),
        name="scores",
    )(parts, target)


def shards(
    hidden,
    wq_direct,
    wkv_direct,
    wo_direct,
    kv_cache,
    parent,
    lengths,
    cand_embed,
    source,
    enc_qkv,
    enc_out,
    cross_q,
    cross_kv,
    cross_out,
    w_direct,
    w_channel,
    target_shard,
):
    bf16 = jnp.bfloat16
    beam_n, len_n, width = cand_embed.shape
    rows_n = beam_n * len_n
    own_start = lax.axis_index(MP) * width
    rows = jnp.concatenate(
        [cand_embed.reshape(rows_n, width), jnp.tile(source[0], (4, 1))], axis=0
    )
    rows_full, qkv_full = gather(
        [rows],
        [dict(chunks=(128, 128, 128, 160), y_time=2.0, z_time=9.0)],
        [enc_qkv],
        [dict(z_time=5.0, x_time=4.0)],
        1,
    )
    query_new = dot(hidden, wq_direct).astype(bf16)
    key_new = dot(hidden, wkv_direct[0]).astype(bf16)
    value_new = dot(hidden, wkv_direct[1]).astype(bf16)
    local = pltpu.VMEM((rows_n, 2 * HD), bf16)
    direct_context = local_call(
        direct_kernel,
        (beam_n, 2 * HD),
        [parent, lengths],
        [query_new, key_new, value_new, kv_cache],
        [local, local],
    )
    tokens_full = rows_full[:rows_n]
    enc = [dot(tokens_full, qkv_full[j]).astype(bf16) for j in range(3)]
    enc_context = local_call(encoder_kernel, (rows_n, 2 * HD), [parent, lengths], enc)
    contexts = jnp.concatenate(
        [enc_context, direct_context, jnp.zeros_like(direct_context)], axis=0
    )
    context_full, out_full, query_full = gather(
        [contexts],
        [dict(chunks=(256, 288), y_time=2.0, z_time=7.0)],
        [enc_out[None], cross_q[None]],
        [dict(z_time=2.0, x_time=1.5), dict(z_time=2.1, x_time=1.6)],
        2,
    )
    hidden_share = lax.dynamic_slice_in_dim(hidden, own_start, width, 1).astype(jnp.float32)
    new_state = hidden_share + dot(context_full[rows_n : rows_n + beam_n], wo_direct)
    tokens = cand_embed[parent].reshape(rows_n, width)
    summed = tokens.astype(jnp.float32) + dot(context_full[:rows_n], out_full[0])
    cross_queries = dot(rows_full[rows_n : rows_n + 8], query_full[0]).astype(bf16)
    summed_full, memory_full, cross_full = gather(
        [summed.astype(bf16)],
        [dict(chunks=(128,) * 4, y_time=2.0, z_time=9.0)],
        [cross_kv, cross_out[None]],
        [dict(z_time=5.0, x_time=3.0), dict(z_time=5.1, x_time=3.1)],
        3,
    )
    wide = summed_full.astype(jnp.float32)
    norm = jnp.sqrt(jnp.mean(wide * wide, axis=1, keepdims=True) + EPSILON)
    cross_keys = (dot(summed_full, memory_full[0]) / norm).astype(bf16)
    cross_values = (dot(summed_full, memory_full[1]) / norm).astype(bf16)
    cross_context = local_call(
        cross_kernel,
        (8 * beam_n, 2 * HD),
        [lengths],
        [jnp.repeat(cross_queries, beam_n, axis=0), cross_keys, cross_values],
    )
    (cross_context_full,) = gather(
        [cross_context], [dict(chunks=(128,), y_time=2.0, z_time=5.0)], [], [], 4
    )
    decoded = dot(cross_context_full, cross_full[0]).reshape(8, beam_n, width)
    decoded = decoded + source[0].astype(jnp.float32)[:, None]
    parts = jnp.concatenate(
        [
            jnp.sum(decoded * w_channel.astype(jnp.float32), axis=2),
            jnp.sum(decoded * decoded, axis=2),
            jnp.sum(new_state * w_direct.astype(jnp.float32), axis=1)[None],
            jnp.sum(new_state * new_state, axis=1)[None],
        ],
        axis=0,
    )
    parts = jnp.pad(parts, ((0, 6), (0, 128 - beam_n)))
    target = jnp.pad(target_shard[None], ((0, 0), (0, 128 - beam_n)), constant_values=-1)
    rerank, channel = scores(parts, target)
    return (new_state.astype(bf16), rerank[0, :beam_n], channel[0, :beam_n])


def solution(mesh):
    split = Mesh(mesh.devices.reshape(ZL, X, Y, ZH, C), AX)
    in_specs = (
        P(DP, None),
        P(None, MP),
        P(None, None, MP),
        P(None, MP),
        P(None, DP, None, MP),
        P(DP),
        P(DP),
        P(DP, None, MP),
        P(DP, None, MP),
        P(None, DP, MP),
        P(DP, MP),
        P(DP, MP),
        P(None, DP, MP),
        P(DP, MP),
        P(MP),
        P(MP),
        P(DP),
    )
    out_specs = (P(DP, MP), P(DP), P(DP))
    return jax.shard_map(
        shards, mesh=split, in_specs=in_specs, out_specs=out_specs, check_vma=False
    )
```

```python
import functools
import math

import jax
import jax.numpy as jnp
from jax import lax
from jax.experimental import pallas as pl
from jax.experimental.pallas import tpu as pltpu
from jax.sharding import Mesh
from jax.sharding import PartitionSpec as P

D = 4096
HD = 64
EPSILON = 1e-06
AX = ("zl", "x", "y", "zh", "c")
ZL, X, Y, ZH, C = 8, 4, 4, 2, 2
MP = ("y", "zh", "c")
DP = ("zl", "x")
VMEM = pltpu.VMEM
LAG = 4
MESH = pl.DeviceIdType.MESH


def hint(value, step):
    return pl.multiple_of(value, step)


def gather_kernel(chunks, plan, n_dp, *refs):
    mp_in, dp_in = refs[0], refs[1 : 1 + n_dp]
    mp_out, dp_out = refs[1 + n_dp], refs[2 + n_dp : 2 + 2 * n_dp]
    send, recv, local = refs[2 + 2 * n_dp :]
    zl, x, y, zh, c = (lax.axis_index(a) for a in AX)
    yr, yl, y2 = lax.rem(y + 1, Y), lax.rem(y + Y - 1, Y), lax.rem(y + 2, Y)
    xr, xl = lax.rem(x + 1, X), lax.rem(x + X - 1, X)
    other = 1 - zh
    to_y = {1: {"y": yr}, -1: {"y": yl}}
    to_x = {1: {"x": xr}, -1: {"x": xl}}
    to_z = {}
    for way in (1, -1):
        near = lax.rem(zh * ZL + zl + way + ZL * ZH, ZL * ZH)
        to_z[way] = {"zh": near // ZL, "zl": lax.rem(near, ZL)}
    to_other = {"zh": other}
    to_partner = {"c": 1 - c}
    width = mp_in.shape[1]
    n = mp_in.shape[0] // chunks
    first = n // 32 * 16

    def column(yy, hh):
        return pl.ds(hint(((yy * ZH + hh) * C + c) * width, 128), width)

    def block(k, b, xx, start, size):
        rows = dp_in[k].shape[1]
        return dp_out[k].at[:, pl.ds(hint((b * X + xx) * rows + start, 16), size)]

    homes = [pltpu.make_async_copy(mp_in, mp_out.at[:, column(y, zh)], local.at[0])]
    for k in range(n_dp):
        homes.append(
            pltpu.make_async_copy(
                dp_in[k], block(k, zl, x, 0, dp_in[k].shape[1]), local.at[1 + k]
            )
        )
    for home in homes:
        home.start()

    barrier = pltpu.get_barrier_semaphore()
    peers = [to_other, to_y[1], to_y[-1], to_partner]
    if n_dp:
        peers += [to_x[1], to_x[-1]]
        peers += [to_z[1], to_z[-1]]
    for peer in peers:
        pl.semaphore_signal(barrier, inc=1, device_id=peer, device_id_type=MESH)
    pl.semaphore_wait(barrier, len(peers))
    for home in homes:
        home.wait()

    def copy(slot, ref, to):
        return pltpu.make_async_remote_copy(
            src_ref=ref,
            dst_ref=ref,
            send_sem=send.at[slot],
            recv_sem=recv.at[slot],
            device_id=to,
            device_id_type=MESH,
        )

    whole, low, high = (0, n), (0, first), (first, n - first)
    table = {
        "z": (whole, y, 0, to_other),
        "r": (whole, y, 1, to_y[1]),
        "l": (whole, y, 1, to_y[-1]),
        "c": (whole, y, 1, to_partner),
        "cl": (whole, yl, 1, to_partner),
        "cr": (whole, yr, 1, to_partner),
        "co": (whole, y2, 1, to_partner),
        "or": (low, yl, 1, to_y[1]),
        "ol": (high, yr, 1, to_y[-1]),
    }
    order = {name: i for i, name in enumerate(table)}
    n_kinds = 2 * len(table)

    def mp_slot(name, phase, j):
        return (order[name] * 2 + phase) * chunks + j

    def flow(name, phase, j):
        (start, size), yy, _, to = table[name]
        hh = lax.rem(zh + phase, ZH)
        rows = pl.ds(hint(j * n + start, 16), size)
        return copy(mp_slot(name, phase, j), mp_out.at[rows, column(yy, hh)], to)

    def loop(start, stop, body):
        def step(j, carry):
            body(j + start)
            return carry

        lax.fori_loop(0, stop - start, step, 0)

    def each(body):
        loop(0, chunks, body)

    def open_phase(phase, j):
        for name in ("r", "l", "c"):
            flow(name, phase, j).start()

    def cross(j):
        flow("z", 0, j).start()

    def open_other(j):
        flow("z", 0, j).wait_recv()
        open_phase(1, j)

    def pass_on(phase, j):
        flow("r", phase, j).wait_recv()
        flow("or", phase, j).start()
        flow("cl", phase, j).start()
        flow("l", phase, j).wait_recv()
        flow("ol", phase, j).start()
        flow("cr", phase, j).start()

    def take_far(phase, j):
        flow("or", phase, j).wait_recv()
        flow("ol", phase, j).wait_recv()
        flow("co", phase, j).start()

    def close_all():
        each(lambda j: flow("z", 0, j).wait_send())

        def close(phase):
            def body(j):
                for name in table:
                    if name != "z":
                        if name[0] == "c":
                            flow(name, phase, j).wait_recv()
                        flow(name, phase, j).wait_send()

            each(body)

        loop(0, 2, close)

    if not n_dp:
        each(cross)
    each(functools.partial(open_phase, 0))
    if not n_dp:

        def phase_step(phase):
            @pl.when(phase == 1)
            def _():
                each(open_other)

            each(functools.partial(pass_on, phase))
            each(functools.partial(take_far, phase))

        loop(0, 2, phase_step)
        close_all()
        return

    z_base = n_kinds * chunks
    x_base = z_base + 2 * ZL * n_dp
    ways = (1, -1)

    def has(way, s):
        return (zl - s >= 0) if way > 0 else ((zl + s <= ZL - 1) & (s >= 1))

    def sends(way, s):
        return (zl - s >= 0) & (zl < ZL - 1) if way > 0 else (zl + s <= ZL - 1) & (zl > 0)

    def held(way, s):
        return lax.rem(zl - way * s + 2 * ZL, ZL)

    def z_flow(way, s, k, b, to):
        slot = z_base + (ZL if way < 0 else 0) * n_dp + s * n_dp + k
        return copy(slot, block(k, b, x, 0, dp_in[k].shape[1]), to)

    def x_flow(way, s, k, kind):
        rows = dp_in[k].shape[1]
        half = rows // 2
        slot = x_base + (((way < 0) * ZL + s) * n_dp + k) * 4 + kind
        b = held(way, s)
        xx, start, size, side = (
            (x, 0, rows, 1),
            (x, 0, rows, -1),
            (xl, 0, half, 1),
            (xr, half, half, -1),
        )[kind]
        return copy(slot, block(k, b, xx, start, size), to_x[side])

    for way in ways:

        @pl.when(sends(way, 0))
        def _():
            for k in range(n_dp):
                z_flow(way, 0, k, zl, to_z[way]).start()

    for k in range(n_dp):
        x_flow(1, 0, k, 0).start()
        x_flow(1, 0, k, 1).start()

    lag = LAG

    def line_step(step, carry):
        beat = step + 1
        s = lax.rem(beat, ZL)
        for way in ways:

            @pl.when((beat <= ZL - 1) & has(way, s))
            def _():
                for k in range(n_dp):
                    z_flow(way, s - 1, k, held(way, s), to_z[-way]).wait_recv()

                    @pl.when((s < ZL - 1) & sends(way, s))
                    def _():
                        z_flow(way, s, k, held(way, s), to_z[way]).start()

                    x_flow(way, s, k, 0).start()
                    x_flow(way, s, k, 1).start()

        t = lax.rem(beat + 2 * ZL - lag, ZL)
        for way in ways:

            @pl.when((beat >= lag) & has(way, t))
            def _():
                for k in range(n_dp):
                    x_flow(way, t, k, 0).wait_recv()
                    x_flow(way, t, k, 2).start()
                    x_flow(way, t, k, 1).wait_recv()
                    x_flow(way, t, k, 3).start()

        pass_0, far_0, go_z, start_1, pass_1, far_1 = plan
        pl.when(beat == go_z)(lambda: each(cross))
        pl.when(beat == start_1)(lambda: each(open_other))

        @pl.when((beat == pass_0) | (beat == pass_1))
        def _():
            each(functools.partial(pass_on, lax.div(beat, pass_1)))

        @pl.when((beat == far_0) | (beat == far_1))
        def _():
            each(functools.partial(take_far, lax.div(beat, far_1)))

        return carry

    lax.fori_loop(0, ZL + lag - 1, line_step, 0)

    def line_close(s, carry):
        for way in ways:

            @pl.when(has(way, s))
            def _():
                for k in range(n_dp):
                    for kind in range(4):
                        if kind > 1:
                            x_flow(way, s, k, kind).wait_recv()
                        x_flow(way, s, k, kind).wait_send()

            @pl.when((s < ZL - 1) & sends(way, s))
            def _():
                for k in range(n_dp):
                    z_flow(way, s, k, held(way, s), to_z[way]).wait_send()

        return carry

    lax.fori_loop(0, ZL, line_close, 0)
    close_all()


def gather(rows, chunks, plan, weights, collective_id):
    outs = [jax.ShapeDtypeStruct((rows.shape[0], rows.shape[1] * 16), rows.dtype)]
    outs += [
        jax.ShapeDtypeStruct((a.shape[0], a.shape[1] * 32, a.shape[2]), a.dtype) for a in weights
    ]
    n_dp = len(weights)
    slots = 18 * chunks + (2 * ZL + 8 * ZL) * n_dp
    return pl.pallas_call(
        functools.partial(gather_kernel, chunks, plan, n_dp),
        out_shape=outs,
        in_specs=[pl.BlockSpec(memory_space=VMEM)] * (1 + n_dp),
        out_specs=[pl.BlockSpec(memory_space=VMEM)] * (1 + n_dp),
        scratch_shapes=[
            pltpu.SemaphoreType.DMA((slots,)),
            pltpu.SemaphoreType.DMA((slots,)),
            pltpu.SemaphoreType.DMA((1 + n_dp,)),
        ],
        compiler_params=pltpu.CompilerParams(
            collective_id=collective_id, has_side_effects=True, vmem_limit_bytes=48 << 20
        ),
        name=f"gather_{collective_id}",
    )(rows, *weights)


def dot(a, b):
    return jnp.dot(a, b, preferred_element_type=jnp.float32)


def dot_t(a, b):
    return lax.dot_general(a, b, (((1,), (1,)), ((), ())), preferred_element_type=jnp.float32)


def of_head(array, head):
    lane = lax.broadcasted_iota(jnp.int32, array.shape, 1)
    return jnp.where((lane >= HD) == (head == 1), array, jnp.zeros_like(array))


def join_heads(first, second):
    lane = lax.broadcasted_iota(jnp.int32, first.shape, 1)
    return jnp.where(lane >= HD, second, first)


def softmax(scores):
    top = jnp.max(scores, axis=1, keepdims=True)
    raised = jnp.exp(scores - top)
    return raised / jnp.sum(raised, axis=1, keepdims=True)


def length_row(lengths, first, count, width):
    col = lax.broadcasted_iota(jnp.int32, (1, width), 1)
    row = jnp.zeros((1, width), jnp.int32)
    for u in range(count):
        row = jnp.where(col // 32 == u, lengths[first + u], row)
    return row


def encoder_kernel(parent, lengths, enc, out):
    group = 4
    for first in range(0, 16, group):
        starts = [hint(parent[first + u] * 32, 32) for u in range(group)]
        queries, keys, values = (
            jnp.concatenate([enc[pl.ds(s, 32), pl.ds(at, 128)] for s in starts], axis=0)
            for at in (0, 128, 256)
        )
        shape = (32 * group, 32 * group)
        row = lax.broadcasted_iota(jnp.int32, shape, 0)
        col = lax.broadcasted_iota(jnp.int32, shape, 1)
        live = (row // 32 == col // 32) & (
            col % 32 < length_row(lengths, first, group, 32 * group)
        )
        heads = []
        for head in range(2):
            scores = dot_t(of_head(queries, head), keys) * (1.0 / math.sqrt(HD))
            weights = softmax(jnp.where(live, scores, -1e30)).astype(jnp.bfloat16)
            heads.append(dot(weights, values))
        out[pl.ds(32 * first, 32 * group), :] = join_heads(*heads).astype(jnp.bfloat16)


def direct_kernel(parent, lengths, q, k, v, cache, out, keys, values):
    for i in range(16):
        keys[pl.ds(32 * i, 32), :] = cache[0, parent[i]]
        values[pl.ds(32 * i, 32), :] = cache[1, parent[i]]
    queries, key_new, value_new = q[...], k[...], v[...].astype(jnp.float32)
    row = lax.broadcasted_iota(jnp.int32, (16, 512), 0)
    col = lax.broadcasted_iota(jnp.int32, (16, 512), 1)
    live = (row == col // 32) & (col % 32 < length_row(lengths, 0, 16, 512))
    heads = []
    for head in range(2):
        mine = of_head(queries, head)
        scores = dot_t(mine, keys[...]) * (1.0 / math.sqrt(HD))
        scores = jnp.where(live, scores, -1e30)
        last = jnp.sum(
            mine.astype(jnp.float32) * key_new.astype(jnp.float32), axis=1, keepdims=True
        ) * (1.0 / math.sqrt(HD))
        top = jnp.maximum(jnp.max(scores, axis=1, keepdims=True), last)
        raised, raised_last = jnp.exp(scores - top), jnp.exp(last - top)
        total = jnp.sum(raised, axis=1, keepdims=True) + raised_last
        weights = (raised / total).astype(jnp.bfloat16)
        weight_last = (raised_last / total).astype(jnp.bfloat16).astype(jnp.float32)
        heads.append(dot(weights, values[...]) + weight_last * value_new)
    out[...] = join_heads(*heads).astype(jnp.bfloat16)


def cross_kernel(lengths, q, kv, out):
    k, v = kv[:, 0:128], kv[:, 128:256]
    row = lax.broadcasted_iota(jnp.int32, (128, 512), 0)
    col = lax.broadcasted_iota(jnp.int32, (128, 512), 1)
    live = (row % 16 == col // 32) & (col % 32 < length_row(lengths, 0, 16, 512))
    heads = []
    for head in range(2):
        scores = dot_t(of_head(q[...], head), k) * (1.0 / math.sqrt(HD))
        weights = softmax(jnp.where(live, scores, -1e30)).astype(jnp.bfloat16)
        heads.append(dot(weights, v))
    out[...] = join_heads(*heads).astype(jnp.bfloat16)


def local_call(kernel, out_shape, scalars, arrays, scratch=()):
    return pl.pallas_call(
        kernel,
        out_shape=jax.ShapeDtypeStruct(out_shape, jnp.bfloat16),
        in_specs=[pl.BlockSpec(memory_space=pltpu.SMEM)] * len(scalars)
        + [pl.BlockSpec(memory_space=VMEM)] * len(arrays),
        out_specs=pl.BlockSpec(memory_space=VMEM),
        scratch_shapes=list(scratch),
    )(*scalars, *arrays)


def score_kernel(parts, target, rerank, channel, got, rows, inbox, sends, recvs):
    zl, x, y, zh, c = (lax.axis_index(a) for a in AX)
    me_m = (y * ZH + zh) * C + c
    me_d = zl * X + x
    n_m, n_d = Y * ZH * C, ZL * X

    def to_m(k):
        m = lax.rem(me_m + k, n_m)
        return {"y": m // (ZH * C), "zh": lax.rem(m // C, ZH), "c": lax.rem(m, C)}

    def to_d(k):
        d = lax.rem(me_d + k, n_d)
        return {"zl": d // X, "x": lax.rem(d, X)}

    def loop(start, stop, body):
        def step(k, carry):
            body(k + start)
            return carry

        lax.fori_loop(0, stop - start, step, 0)

    barrier = pltpu.get_barrier_semaphore()

    def greet(to):
        pl.semaphore_signal(barrier, inc=1, device_id=to, device_id_type=MESH)

    loop(1, n_m, lambda k: greet(to_m(k)))
    loop(1, n_d, lambda k: greet(to_d(k)))
    pl.semaphore_wait(barrier, n_m + n_d - 2)

    def part_flow(k):
        return pltpu.make_async_remote_copy(
            src_ref=parts,
            dst_ref=got.at[me_m],
            send_sem=sends.at[k],
            recv_sem=recvs.at[k],
            device_id=to_m(k),
            device_id_type=MESH,
        )

    def score_flow(k):
        return pltpu.make_async_remote_copy(
            src_ref=rows.at[pl.ds(lax.rem(me_d + k, n_d), 1)],
            dst_ref=inbox.at[pl.ds(me_d, 1)],
            send_sem=sends.at[n_m + k],
            recv_sem=recvs.at[n_m + k],
            device_id=to_d(k),
            device_id_type=MESH,
        )

    loop(1, n_m, lambda k: part_flow(k).start())
    loop(1, n_m, lambda k: part_flow(k).wait_recv())
    total = parts[...]
    for m in range(n_m):
        total = total + jnp.where(me_m == m, 0.0, got[m])
    each = total[0:1] / jnp.sqrt(total[1:2] / D + EPSILON)
    lane = lax.broadcasted_iota(jnp.int32, (128, 128), 0)
    slot = lax.broadcasted_iota(jnp.int32, (128, 128), 1)
    pick = jnp.where(lane % 16 == slot, 1.0, 0.0)
    score = jnp.dot(
        jnp.broadcast_to(each, (8, 128)),
        pick,
        precision=lax.Precision.HIGHEST,
        preferred_element_type=jnp.float32,
    )[0:1] * (1.0 / 8)
    direct = total[2:3] / jnp.sqrt(total[3:4] / D + EPSILON)
    rerank[...] = direct + score
    shard = lax.broadcasted_iota(jnp.int32, (n_d, 128), 0)
    slots = jnp.where(shard == target[...], score, 0.0)
    rows[...] = slots
    loop(1, n_d, lambda k: score_flow(k).start())
    loop(1, n_d, lambda k: score_flow(k).wait_recv())
    mine = shard == me_d
    channel[...] = jnp.sum(jnp.where(mine, slots, inbox[...]), axis=0, keepdims=True)
    loop(1, n_m, lambda k: part_flow(k).wait_send())
    loop(1, n_d, lambda k: score_flow(k).wait_send())


def scores(parts, target):
    return pl.pallas_call(
        score_kernel,
        out_shape=[jax.ShapeDtypeStruct((1, 128), jnp.float32)] * 2,
        in_specs=[pl.BlockSpec(memory_space=VMEM)] * 2,
        out_specs=[pl.BlockSpec(memory_space=VMEM)] * 2,
        scratch_shapes=[
            pltpu.VMEM((16, 4, 128), jnp.float32),
            pltpu.VMEM((32, 128), jnp.float32),
            pltpu.VMEM((32, 128), jnp.float32),
            pltpu.SemaphoreType.DMA((48,)),
            pltpu.SemaphoreType.DMA((48,)),
        ],
        compiler_params=pltpu.CompilerParams(collective_id=9, has_side_effects=True),
        name="scores",
    )(parts, target)


def folded(weight):
    return jnp.concatenate([weight[:, :128], weight[:, 128:]], axis=0)


def unfolded_dot(rows, weight):
    blocks = weight.reshape(ZL * X, 2, -1, 128)
    halves = [dot(rows, blocks[:, h].reshape(-1, 128)) for h in range(2)]
    return jnp.concatenate(halves, axis=1)


def shards(
    hidden,
    wq_direct,
    wkv_direct,
    wo_direct,
    kv_cache,
    parent,
    lengths,
    cand_embed,
    source,
    enc_qkv,
    enc_out,
    cross_q,
    cross_kv,
    cross_out,
    w_direct,
    w_channel,
    target_shard,
):
    bf16 = jnp.bfloat16
    beam_n, len_n, width = cand_embed.shape
    rows_n = beam_n * len_n
    own_start = lax.axis_index(MP) * width
    rows = jnp.concatenate(
        [cand_embed.reshape(rows_n, width), jnp.tile(source[0], (2, 1))], axis=0
    )
    first_pack = jnp.concatenate([enc_qkv[0], enc_qkv[1], enc_qkv[2], cross_q, folded(enc_out)], 1)
    second_pack = jnp.concatenate([cross_kv[0], cross_kv[1], folded(cross_out)], 1)
    rows_full, first_full, second_full = gather(
        rows, 3, (1, 2, 5, 8, 9, 10), [first_pack[None], second_pack[None]], 1
    )
    query_new = dot(hidden, wq_direct).astype(bf16)
    key_new = dot(hidden, wkv_direct[0]).astype(bf16)
    value_new = dot(hidden, wkv_direct[1]).astype(bf16)
    local = pltpu.VMEM((rows_n, 2 * HD), bf16)
    direct_context = local_call(
        direct_kernel,
        (beam_n, 2 * HD),
        [parent, lengths],
        [query_new, key_new, value_new, kv_cache],
        [local, local],
    )
    enc = dot(rows_full, first_full[0]).astype(bf16)
    enc_context = local_call(encoder_kernel, (rows_n, 2 * HD), [parent, lengths], [enc])
    contexts = jnp.concatenate([enc_context, direct_context], axis=0)
    (context_full,) = gather(contexts, 3, (), [], 2)
    hidden_share = lax.dynamic_slice_in_dim(hidden, own_start, width, 1).astype(jnp.float32)
    new_state = hidden_share + dot(context_full[rows_n : rows_n + beam_n], wo_direct)
    tokens = cand_embed[parent].reshape(rows_n, width)
    summed = tokens.astype(jnp.float32) + unfolded_dot(
        context_full[:rows_n], first_full[0, :, 4 * 2 * HD :]
    )
    cross_queries = enc[rows_n : rows_n + 8, 3 * 2 * HD : 4 * 2 * HD]
    (summed_full,) = gather(summed.astype(bf16), 4, (), [], 3)
    wide = summed_full.astype(jnp.float32)
    norm = jnp.sqrt(jnp.mean(wide * wide, axis=1, keepdims=True) + EPSILON)
    keys_values = (dot(summed_full, second_full[0, :, : 4 * HD]) / norm).astype(bf16)
    cross_context = local_call(
        cross_kernel,
        (8 * beam_n, 2 * HD),
        [lengths],
        [jnp.repeat(cross_queries, beam_n, axis=0), keys_values],
    )
    (cross_context_full,) = gather(cross_context, 1, (), [], 4)
    decoded = unfolded_dot(cross_context_full, second_full[0, :, 4 * HD :])
    decoded = decoded + jnp.repeat(source[0].astype(jnp.float32), beam_n, axis=0)
    lanes = ((0, 128 - beam_n),)
    parts = jnp.stack(
        [
            jnp.sum(decoded * w_channel.astype(jnp.float32), axis=1),
            jnp.sum(decoded * decoded, axis=1),
            jnp.pad(jnp.sum(new_state * w_direct.astype(jnp.float32), axis=1), lanes),
            jnp.pad(jnp.sum(new_state * new_state, axis=1), lanes),
        ]
    )
    target = jnp.pad(target_shard[None], ((0, 0), (0, 128 - beam_n)), constant_values=-1)
    rerank, channel = scores(parts, target)
    return (new_state.astype(bf16), rerank[0, :beam_n], channel[0, :beam_n])


def solution(mesh):
    split = Mesh(mesh.devices.reshape(ZL, X, Y, ZH, C), AX)
    in_specs = (
        P(DP, None),
        P(None, MP),
        P(None, None, MP),
        P(None, MP),
        P(None, DP, None, MP),
        P(DP),
        P(DP),
        P(DP, None, MP),
        P(DP, None, MP),
        P(None, DP, MP),
        P(DP, MP),
        P(DP, MP),
        P(None, DP, MP),
        P(DP, MP),
        P(MP),
        P(MP),
        P(DP),
    )
    out_specs = (P(DP, MP), P(DP), P(DP))
    return jax.shard_map(
        shards, mesh=split, in_specs=in_specs, out_specs=out_specs, check_vma=False
    )
```

```python
import functools
import math

import jax
import jax.numpy as jnp
from jax import lax
from jax.experimental import pallas as pl
from jax.experimental.pallas import tpu as pltpu
from jax.sharding import Mesh
from jax.sharding import PartitionSpec as P

D = 4096
HD = 64
EPSILON = 1e-06
AX = ("zl", "x", "y", "zh", "c")
ZL, X, Y, ZH, C = 8, 4, 4, 2, 2
MP = ("y", "zh", "c")
DP = ("zl", "x")
VMEM = pltpu.VMEM
LAG = 4
MESH = pl.DeviceIdType.MESH


def hint(value, step):
    return pl.multiple_of(value, step)


def gather_kernel(chunks, plan, n_dp, *refs):
    mp_in, dp_in = refs[0], refs[1 : 1 + n_dp]
    mp_out, dp_out = refs[1 + n_dp], refs[2 + n_dp : 2 + 2 * n_dp]
    send, recv, local = refs[2 + 2 * n_dp :]
    zl, x, y, zh, c = (lax.axis_index(a) for a in AX)
    yr, yl, y2 = lax.rem(y + 1, Y), lax.rem(y + Y - 1, Y), lax.rem(y + 2, Y)
    xr, xl = lax.rem(x + 1, X), lax.rem(x + X - 1, X)
    other = 1 - zh
    to_y = {1: {"y": yr}, -1: {"y": yl}}
    to_x = {1: {"x": xr}, -1: {"x": xl}}
    to_z = {}
    for way in (1, -1):
        near = lax.rem(zh * ZL + zl + way + ZL * ZH, ZL * ZH)
        to_z[way] = {"zh": near // ZL, "zl": lax.rem(near, ZL)}
    to_other = {"zh": other}
    to_partner = {"c": 1 - c}
    width = mp_in.shape[1]
    n = mp_in.shape[0] // chunks
    first = n // 32 * 16

    def column(yy, hh):
        return pl.ds(hint(((yy * ZH + hh) * C + c) * width, 128), width)

    def block(k, b, xx, start, size):
        rows = dp_in[k].shape[1]
        return dp_out[k].at[:, pl.ds(hint((b * X + xx) * rows + start, 16), size)]

    homes = [pltpu.make_async_copy(mp_in, mp_out.at[:, column(y, zh)], local.at[0])]
    for k in range(n_dp):
        homes.append(
            pltpu.make_async_copy(
                dp_in[k], block(k, zl, x, 0, dp_in[k].shape[1]), local.at[1 + k]
            )
        )
    for home in homes:
        home.start()

    barrier = pltpu.get_barrier_semaphore()
    peers = [to_other, to_y[1], to_y[-1], to_partner]
    if n_dp:
        peers += [to_x[1], to_x[-1]]
        peers += [to_z[1], to_z[-1]]
    for peer in peers:
        pl.semaphore_signal(barrier, inc=1, device_id=peer, device_id_type=MESH)
    pl.semaphore_wait(barrier, len(peers))
    for home in homes:
        home.wait()

    def copy(slot, ref, to):
        return pltpu.make_async_remote_copy(
            src_ref=ref,
            dst_ref=ref,
            send_sem=send.at[slot],
            recv_sem=recv.at[slot],
            device_id=to,
            device_id_type=MESH,
        )

    whole, low, high = (0, n), (0, first), (first, n - first)
    table = {
        "z": (whole, y, 0, to_other),
        "r": (whole, y, 1, to_y[1]),
        "l": (whole, y, 1, to_y[-1]),
        "c": (whole, y, 1, to_partner),
        "cl": (whole, yl, 1, to_partner),
        "cr": (whole, yr, 1, to_partner),
        "co": (whole, y2, 1, to_partner),
        "or": (low, yl, 1, to_y[1]),
        "ol": (high, yr, 1, to_y[-1]),
    }
    order = {name: i for i, name in enumerate(table)}
    n_kinds = 2 * len(table)

    def mp_slot(name, phase, j):
        return (order[name] * 2 + phase) * chunks + j

    def flow(name, phase, j):
        (start, size), yy, _, to = table[name]
        hh = lax.rem(zh + phase, ZH)
        rows = pl.ds(hint(j * n + start, 16), size)
        return copy(mp_slot(name, phase, j), mp_out.at[rows, column(yy, hh)], to)

    def loop(start, stop, body):
        def step(j, carry):
            body(j + start)
            return carry

        lax.fori_loop(0, stop - start, step, 0)

    def each(body):
        loop(0, chunks, body)

    def open_phase(phase, j):
        for name in ("r", "l", "c"):
            flow(name, phase, j).start()

    def cross(j):
        flow("z", 0, j).start()

    def open_other(j):
        flow("z", 0, j).wait_recv()
        open_phase(1, j)

    def pass_on(phase, j):
        flow("r", phase, j).wait_recv()
        flow("or", phase, j).start()
        flow("cl", phase, j).start()
        flow("l", phase, j).wait_recv()
        flow("ol", phase, j).start()
        flow("cr", phase, j).start()

    def take_far(phase, j):
        flow("or", phase, j).wait_recv()
        flow("ol", phase, j).wait_recv()
        flow("co", phase, j).start()

    def close_all():
        each(lambda j: flow("z", 0, j).wait_send())

        def close(phase):
            def body(j):
                for name in table:
                    if name != "z":
                        if name[0] == "c":
                            flow(name, phase, j).wait_recv()
                        flow(name, phase, j).wait_send()

            each(body)

        loop(0, 2, close)

    if not n_dp:
        each(cross)
    each(functools.partial(open_phase, 0))
    if not n_dp:

        def phase_step(phase):
            @pl.when(phase == 1)
            def _():
                each(open_other)

            each(functools.partial(pass_on, phase))
            each(functools.partial(take_far, phase))

        loop(0, 2, phase_step)
        close_all()
        return

    z_base = n_kinds * chunks
    x_base = z_base + 2 * ZL * n_dp
    ways = (1, -1)

    def has(way, s):
        return (zl - s >= 0) if way > 0 else ((zl + s <= ZL - 1) & (s >= 1))

    def sends(way, s):
        return (zl - s >= 0) & (zl < ZL - 1) if way > 0 else (zl + s <= ZL - 1) & (zl > 0)

    def held(way, s):
        return lax.rem(zl - way * s + 2 * ZL, ZL)

    def z_flow(way, s, k, b, to):
        slot = z_base + (ZL if way < 0 else 0) * n_dp + s * n_dp + k
        return copy(slot, block(k, b, x, 0, dp_in[k].shape[1]), to)

    def x_flow(way, s, k, kind):
        rows = dp_in[k].shape[1]
        half = rows // 2
        slot = x_base + (((way < 0) * ZL + s) * n_dp + k) * 4 + kind
        b = held(way, s)
        xx, start, size, side = (
            (x, 0, rows, 1),
            (x, 0, rows, -1),
            (xl, 0, half, 1),
            (xr, half, half, -1),
        )[kind]
        return copy(slot, block(k, b, xx, start, size), to_x[side])

    for way in ways:

        @pl.when(sends(way, 0))
        def _():
            for k in range(n_dp):
                z_flow(way, 0, k, zl, to_z[way]).start()

    for k in range(n_dp):
        x_flow(1, 0, k, 0).start()
        x_flow(1, 0, k, 1).start()

    lag = LAG

    def line_step(step, carry):
        beat = step + 1
        s = lax.rem(beat, ZL)
        for way in ways:

            @pl.when((beat <= ZL - 1) & has(way, s))
            def _():
                for k in range(n_dp):
                    z_flow(way, s - 1, k, held(way, s), to_z[-way]).wait_recv()

                    @pl.when((s < ZL - 1) & sends(way, s))
                    def _():
                        z_flow(way, s, k, held(way, s), to_z[way]).start()

                    x_flow(way, s, k, 0).start()
                    x_flow(way, s, k, 1).start()

        t = lax.rem(beat + 2 * ZL - lag, ZL)
        for way in ways:

            @pl.when((beat >= lag) & has(way, t))
            def _():
                for k in range(n_dp):
                    x_flow(way, t, k, 0).wait_recv()
                    x_flow(way, t, k, 2).start()
                    x_flow(way, t, k, 1).wait_recv()
                    x_flow(way, t, k, 3).start()

        pass_0, far_0, go_z, start_1, pass_1, far_1 = plan
        pl.when(beat == go_z)(lambda: each(cross))
        pl.when(beat == start_1)(lambda: each(open_other))

        @pl.when((beat == pass_0) | (beat == pass_1))
        def _():
            each(functools.partial(pass_on, lax.div(beat, pass_1)))

        @pl.when((beat == far_0) | (beat == far_1))
        def _():
            each(functools.partial(take_far, lax.div(beat, far_1)))

        return carry

    lax.fori_loop(0, ZL + lag - 1, line_step, 0)

    def line_close(s, carry):
        for way in ways:

            @pl.when(has(way, s))
            def _():
                for k in range(n_dp):
                    for kind in range(4):
                        if kind > 1:
                            x_flow(way, s, k, kind).wait_recv()
                        x_flow(way, s, k, kind).wait_send()

            @pl.when((s < ZL - 1) & sends(way, s))
            def _():
                for k in range(n_dp):
                    z_flow(way, s, k, held(way, s), to_z[way]).wait_send()

        return carry

    lax.fori_loop(0, ZL, line_close, 0)
    close_all()


def gather(rows, chunks, plan, weights, collective_id):
    outs = [jax.ShapeDtypeStruct((rows.shape[0], rows.shape[1] * 16), rows.dtype)]
    outs += [
        jax.ShapeDtypeStruct((a.shape[0], a.shape[1] * 32, a.shape[2]), a.dtype) for a in weights
    ]
    n_dp = len(weights)
    slots = 18 * chunks + (2 * ZL + 8 * ZL) * n_dp
    return pl.pallas_call(
        functools.partial(gather_kernel, chunks, plan, n_dp),
        out_shape=outs,
        in_specs=[pl.BlockSpec(memory_space=VMEM)] * (1 + n_dp),
        out_specs=[pl.BlockSpec(memory_space=VMEM)] * (1 + n_dp),
        scratch_shapes=[
            pltpu.SemaphoreType.DMA((slots,)),
            pltpu.SemaphoreType.DMA((slots,)),
            pltpu.SemaphoreType.DMA((1 + n_dp,)),
        ],
        compiler_params=pltpu.CompilerParams(
            collective_id=collective_id, has_side_effects=True, vmem_limit_bytes=48 << 20
        ),
        name=f"gather_{collective_id}",
    )(rows, *weights)


def dot(a, b):
    return jnp.dot(a, b, preferred_element_type=jnp.float32)


def dot_t(a, b):
    return lax.dot_general(a, b, (((1,), (1,)), ((), ())), preferred_element_type=jnp.float32)


def of_head(array, head):
    lane = lax.broadcasted_iota(jnp.int32, array.shape, 1)
    return jnp.where((lane >= HD) == (head == 1), array, jnp.zeros_like(array))


def join_heads(first, second):
    lane = lax.broadcasted_iota(jnp.int32, first.shape, 1)
    return jnp.where(lane >= HD, second, first)


def softmax(scores):
    top = jnp.max(scores, axis=1, keepdims=True)
    raised = jnp.exp(scores - top)
    return raised / jnp.sum(raised, axis=1, keepdims=True)


def length_row(lengths, first, count, width):
    col = lax.broadcasted_iota(jnp.int32, (1, width), 1)
    row = jnp.zeros((1, width), jnp.int32)
    for u in range(count):
        row = jnp.where(col // 32 == u, lengths[first + u], row)
    return row


def encoder_kernel(parent, lengths, enc, out):
    group = 4
    for first in range(0, 16, group):
        starts = [hint(parent[first + u] * 32, 32) for u in range(group)]
        queries, keys, values = (
            jnp.concatenate([enc[pl.ds(s, 32), pl.ds(at, 128)] for s in starts], axis=0)
            for at in (0, 128, 256)
        )
        shape = (32 * group, 32 * group)
        row = lax.broadcasted_iota(jnp.int32, shape, 0)
        col = lax.broadcasted_iota(jnp.int32, shape, 1)
        live = (row // 32 == col // 32) & (
            col % 32 < length_row(lengths, first, group, 32 * group)
        )
        heads = []
        for head in range(2):
            scores = dot_t(of_head(queries, head), keys) * (1.0 / math.sqrt(HD))
            weights = softmax(jnp.where(live, scores, -1e30)).astype(jnp.bfloat16)
            heads.append(dot(weights, values))
        out[pl.ds(32 * first, 32 * group), :] = join_heads(*heads).astype(jnp.bfloat16)


def direct_kernel(parent, lengths, q, k, v, cache, out, keys, values):
    for i in range(16):
        keys[pl.ds(32 * i, 32), :] = cache[0, parent[i]]
        values[pl.ds(32 * i, 32), :] = cache[1, parent[i]]
    queries, key_new, value_new = q[...], k[...], v[...].astype(jnp.float32)
    row = lax.broadcasted_iota(jnp.int32, (16, 512), 0)
    col = lax.broadcasted_iota(jnp.int32, (16, 512), 1)
    live = (row == col // 32) & (col % 32 < length_row(lengths, 0, 16, 512))
    heads = []
    for head in range(2):
        mine = of_head(queries, head)
        scores = dot_t(mine, keys[...]) * (1.0 / math.sqrt(HD))
        scores = jnp.where(live, scores, -1e30)
        last = jnp.sum(
            mine.astype(jnp.float32) * key_new.astype(jnp.float32), axis=1, keepdims=True
        ) * (1.0 / math.sqrt(HD))
        top = jnp.maximum(jnp.max(scores, axis=1, keepdims=True), last)
        raised, raised_last = jnp.exp(scores - top), jnp.exp(last - top)
        total = jnp.sum(raised, axis=1, keepdims=True) + raised_last
        weights = (raised / total).astype(jnp.bfloat16)
        weight_last = (raised_last / total).astype(jnp.bfloat16).astype(jnp.float32)
        heads.append(dot(weights, values[...]) + weight_last * value_new)
    out[...] = join_heads(*heads).astype(jnp.bfloat16)


def cross_kernel(lengths, q, kv, out):
    k, v = kv[:, 0:128], kv[:, 128:256]
    row = lax.broadcasted_iota(jnp.int32, (128, 512), 0)
    col = lax.broadcasted_iota(jnp.int32, (128, 512), 1)
    live = (row % 16 == col // 32) & (col % 32 < length_row(lengths, 0, 16, 512))
    heads = []
    for head in range(2):
        scores = dot_t(of_head(q[...], head), k) * (1.0 / math.sqrt(HD))
        weights = softmax(jnp.where(live, scores, -1e30)).astype(jnp.bfloat16)
        heads.append(dot(weights, v))
    out[...] = join_heads(*heads).astype(jnp.bfloat16)


def local_call(kernel, out_shape, scalars, arrays, scratch=()):
    return pl.pallas_call(
        kernel,
        out_shape=jax.ShapeDtypeStruct(out_shape, jnp.bfloat16),
        in_specs=[pl.BlockSpec(memory_space=pltpu.SMEM)] * len(scalars)
        + [pl.BlockSpec(memory_space=VMEM)] * len(arrays),
        out_specs=pl.BlockSpec(memory_space=VMEM),
        scratch_shapes=list(scratch),
    )(*scalars, *arrays)


def score_kernel(parts, target, rerank, channel, got, rows, inbox, sends, recvs):
    zl, x, y, zh, c = (lax.axis_index(a) for a in AX)
    me_m = (y * ZH + zh) * C + c
    me_d = zl * X + x
    n_m, n_d = Y * ZH * C, ZL * X

    def to_m(k):
        m = lax.rem(me_m + k, n_m)
        return {"y": m // (ZH * C), "zh": lax.rem(m // C, ZH), "c": lax.rem(m, C)}

    def to_d(k):
        d = lax.rem(me_d + k, n_d)
        return {"zl": d // X, "x": lax.rem(d, X)}

    def loop(start, stop, body):
        def step(k, carry):
            body(k + start)
            return carry

        lax.fori_loop(0, stop - start, step, 0)

    barrier = pltpu.get_barrier_semaphore()

    def greet(to):
        pl.semaphore_signal(barrier, inc=1, device_id=to, device_id_type=MESH)

    loop(1, n_m, lambda k: greet(to_m(k)))
    loop(1, n_d, lambda k: greet(to_d(k)))
    pl.semaphore_wait(barrier, n_m + n_d - 2)

    def part_flow(k):
        return pltpu.make_async_remote_copy(
            src_ref=parts,
            dst_ref=got.at[me_m],
            send_sem=sends.at[k],
            recv_sem=recvs.at[k],
            device_id=to_m(k),
            device_id_type=MESH,
        )

    def score_flow(k):
        return pltpu.make_async_remote_copy(
            src_ref=rows.at[pl.ds(lax.rem(me_d + k, n_d), 1)],
            dst_ref=inbox.at[pl.ds(me_d, 1)],
            send_sem=sends.at[n_m + k],
            recv_sem=recvs.at[n_m + k],
            device_id=to_d(k),
            device_id_type=MESH,
        )

    loop(1, n_m, lambda k: part_flow(k).start())
    loop(1, n_m, lambda k: part_flow(k).wait_recv())
    total = parts[...]
    for m in range(n_m):
        total = total + jnp.where(me_m == m, 0.0, got[m])
    each = total[0:1] / jnp.sqrt(total[1:2] / D + EPSILON)
    lane = lax.broadcasted_iota(jnp.int32, (128, 128), 0)
    slot = lax.broadcasted_iota(jnp.int32, (128, 128), 1)
    pick = jnp.where(lane % 16 == slot, 1.0, 0.0)
    score = jnp.dot(
        jnp.broadcast_to(each, (8, 128)),
        pick,
        precision=lax.Precision.HIGHEST,
        preferred_element_type=jnp.float32,
    )[0:1] * (1.0 / 8)
    direct = total[2:3] / jnp.sqrt(total[3:4] / D + EPSILON)
    rerank[...] = direct + score
    shard = lax.broadcasted_iota(jnp.int32, (n_d, 128), 0)
    slots = jnp.where(shard == target[...], score, 0.0)
    rows[...] = slots
    loop(1, n_d, lambda k: score_flow(k).start())
    loop(1, n_d, lambda k: score_flow(k).wait_recv())
    mine = shard == me_d
    channel[...] = jnp.sum(jnp.where(mine, slots, inbox[...]), axis=0, keepdims=True)
    loop(1, n_m, lambda k: part_flow(k).wait_send())
    loop(1, n_d, lambda k: score_flow(k).wait_send())


def scores(parts, target):
    return pl.pallas_call(
        score_kernel,
        out_shape=[jax.ShapeDtypeStruct((1, 128), jnp.float32)] * 2,
        in_specs=[pl.BlockSpec(memory_space=VMEM)] * 2,
        out_specs=[pl.BlockSpec(memory_space=VMEM)] * 2,
        scratch_shapes=[
            pltpu.VMEM((16, 4, 128), jnp.float32),
            pltpu.VMEM((32, 128), jnp.float32),
            pltpu.VMEM((32, 128), jnp.float32),
            pltpu.SemaphoreType.DMA((48,)),
            pltpu.SemaphoreType.DMA((48,)),
        ],
        compiler_params=pltpu.CompilerParams(collective_id=9, has_side_effects=True),
        name="scores",
    )(parts, target)


def folded(weight):
    return jnp.concatenate([weight[:, :128], weight[:, 128:]], axis=0)


def unfolded_dot(rows, weight):
    blocks = weight.reshape(ZL * X, 2, -1, 128)
    halves = [dot(rows, blocks[:, h].reshape(-1, 128)) for h in range(2)]
    return jnp.concatenate(halves, axis=1)


def shards(
    hidden,
    wq_direct,
    wkv_direct,
    wo_direct,
    kv_cache,
    parent,
    lengths,
    cand_embed,
    source,
    enc_qkv,
    enc_out,
    cross_q,
    cross_kv,
    cross_out,
    w_direct,
    w_channel,
    target_shard,
):
    bf16 = jnp.bfloat16
    beam_n, len_n, width = cand_embed.shape
    rows_n = beam_n * len_n
    own_start = lax.axis_index(MP) * width
    rows = jnp.concatenate(
        [cand_embed.reshape(rows_n, width), jnp.tile(source[0], (2, 1))], axis=0
    )
    first_pack = jnp.concatenate([enc_qkv[0], enc_qkv[1], enc_qkv[2], cross_q, folded(enc_out)], 1)
    second_pack = jnp.concatenate([cross_kv[0], cross_kv[1], folded(cross_out)], 1)
    rows_full, first_full, second_full = gather(
        rows, 3, (1, 2, 4, 9, 10, 11), [first_pack[None], second_pack[None]], 1
    )
    query_new = dot(hidden, wq_direct).astype(bf16)
    key_new = dot(hidden, wkv_direct[0]).astype(bf16)
    value_new = dot(hidden, wkv_direct[1]).astype(bf16)
    local = pltpu.VMEM((rows_n, 2 * HD), bf16)
    direct_context = local_call(
        direct_kernel,
        (beam_n, 2 * HD),
        [parent, lengths],
        [query_new, key_new, value_new, kv_cache],
        [local, local],
    )
    enc = dot(rows_full, first_full[0]).astype(bf16)
    enc_context = local_call(encoder_kernel, (rows_n, 2 * HD), [parent, lengths], [enc])
    contexts = jnp.concatenate([enc_context, direct_context], axis=0)
    (context_full,) = gather(contexts, 3, (), [], 2)
    hidden_share = lax.dynamic_slice_in_dim(hidden, own_start, width, 1).astype(jnp.float32)
    new_state = hidden_share + dot(context_full[rows_n : rows_n + beam_n], wo_direct)
    tokens = cand_embed[parent].reshape(rows_n, width)
    summed = tokens.astype(jnp.float32) + unfolded_dot(
        context_full[:rows_n], first_full[0, :, 4 * 2 * HD :]
    )
    cross_queries = enc[rows_n : rows_n + 8, 3 * 2 * HD : 4 * 2 * HD]
    (summed_full,) = gather(summed.astype(bf16), 4, (), [], 3)
    wide = summed_full.astype(jnp.float32)
    norm = jnp.sqrt(jnp.mean(wide * wide, axis=1, keepdims=True) + EPSILON)
    keys_values = (dot(summed_full, second_full[0, :, : 4 * HD]) / norm).astype(bf16)
    cross_context = local_call(
        cross_kernel,
        (8 * beam_n, 2 * HD),
        [lengths],
        [jnp.repeat(cross_queries, beam_n, axis=0), keys_values],
    )
    (cross_context_full,) = gather(cross_context, 1, (), [], 4)
    decoded = unfolded_dot(cross_context_full, second_full[0, :, 4 * HD :])
    decoded = decoded + jnp.repeat(source[0].astype(jnp.float32), beam_n, axis=0)
    lanes = ((0, 128 - beam_n),)
    parts = jnp.stack(
        [
            jnp.sum(decoded * w_channel.astype(jnp.float32), axis=1),
            jnp.sum(decoded * decoded, axis=1),
            jnp.pad(jnp.sum(new_state * w_direct.astype(jnp.float32), axis=1), lanes),
            jnp.pad(jnp.sum(new_state * new_state, axis=1), lanes),
        ]
    )
    target = jnp.pad(target_shard[None], ((0, 0), (0, 128 - beam_n)), constant_values=-1)
    rerank, channel = scores(parts, target)
    return (new_state.astype(bf16), rerank[0, :beam_n], channel[0, :beam_n])


def solution(mesh):
    split = Mesh(mesh.devices.reshape(ZL, X, Y, ZH, C), AX)
    in_specs = (
        P(DP, None),
        P(None, MP),
        P(None, None, MP),
        P(None, MP),
        P(None, DP, None, MP),
        P(DP),
        P(DP),
        P(DP, None, MP),
        P(DP, None, MP),
        P(None, DP, MP),
        P(DP, MP),
        P(DP, MP),
        P(None, DP, MP),
        P(DP, MP),
        P(MP),
        P(MP),
        P(DP),
    )
    out_specs = (P(DP, MP), P(DP), P(DP))
    return jax.shard_map(
        shards, mesh=split, in_specs=in_specs, out_specs=out_specs, check_vma=False
    )
```
